256 devices in a mesh: section: 16 (over y, z_hi), tp: 16 (over x, z_lo, core).
Axes of the slice: x: 4, y: 4, z: 8 (z_hi: 4, z_lo: 2; z = z_hi * 2 + z_lo), core: 2. Of those that a mesh axis runs over, the one named last changes fastest.
Arguments:
- incoming: bfloat16 [16, 256, 6144], P('section', 'tp'), may hold values from -11 to 11, as said below
- grad_in: bfloat16 [16, 256, 6144], P('section', 'tp'), may hold values from -6 to 6
- held: bfloat16 [16, 2, 256, 6144], P('section', None, 'tp'), may hold values from -11 to 11, as said below
- roster: int32 [16, 2], replicated, may hold values from 0 to 1
- norm_gain: float32 [16, 6144], P('section'), may hold values from 0.25 to 1.75
- r_scores: float32 [16, 48, 256, 256], P('section', 'tp'), may hold values from -12 to 236
- value_weight: bfloat16 [16, 6144, 6144], P('section', None, 'tp'), may hold values from -0.078125 to 0.078125
- out_weight: bfloat16 [16, 6144, 6144], P('section', 'tp'), may hold values from -0.078125 to 0.078125
Outputs:
- act_out: bfloat16 [16, 256, 6144], P('section', 'tp')
- grad_out: bfloat16 [16, 256, 6144], P('section', 'tp')
- held_next: bfloat16 [16, 2, 256, 6144], P('section', None, 'tp')
The draws below stay inside these ranges and needn't reach their ends.
Inputs may be any that keep to these rules, and one draw needn't show every extreme that they name: `incoming`: every token row has its own scale. `held`: every token row has its own scale. roster[s, 0] names the slot at section 15 - s that holds section s's stash to fetch; roster[s, 1] names the slot there that takes section s's evicted input; the two may be equal.
All inputs are finite; a program needn't handle non-finite values.
Results may differ from the reference program's by a relative error of at most 0.0036.
Values may be sent and summed in bfloat16 or wider, within the bound.
No kernel may reach another device: no remote copies, remote signals or barrier semaphores. Data moves between devices by JAX's collectives and lax.ppermute only.
A program may use at most 64 MiB of HBM per device.

```python
import math
import jax
import jax.numpy as jnp
from jax import lax

D = 6144
HEADS = 48
HEAD = 128
TOKENS = 256
SLOTS = 2
SECTIONS = 16


def scaled_rows(key, shape):
    first_key, second_key = jax.random.split(key)
    row_shape = shape[:-1] + (1,)
    base = jnp.clip(jax.random.normal(first_key, shape, jnp.float32), -5.5, 5.5)
    scales = jnp.exp(jax.random.uniform(second_key, row_shape, jnp.float32, math.log(0.25), math.log(2.0)))
    return base * scales


def draw_incoming(key, part):
    return scaled_rows(jax.random.fold_in(key, 11), (SECTIONS, TOKENS, D)).astype(jnp.bfloat16)


def draw_held(key, part):
    return scaled_rows(jax.random.fold_in(key, 12), (SECTIONS, SLOTS, TOKENS, D)).astype(jnp.bfloat16)


def draw_r_scores(key, part):
    first_key = jax.random.fold_in(jax.random.fold_in(key, 13), 0)
    shape = (SECTIONS, HEADS, TOKENS, TOKENS)
    return jnp.clip(2.0 * jax.random.normal(first_key, shape, jnp.float32), -12.0, 12.0)


def with_ends(result, rng, smallest, top_value):
    extent = result.shape
    index_at = [jax.random.randint(jax.random.fold_in(rng, axis), (), 0, extent[axis]) for axis in range(len(extent))]
    result = result.at[tuple(index_at)].set(smallest)
    longest = extent.index(max(extent))
    index_at[longest] = (index_at[longest] + 1) % extent[longest]
    return result.at[tuple(index_at)].set(top_value)


def block_scale(own_key, extent, shards, smallest, high):
    loudness = 1.0
    for dim, shards_of in shards:
        heights = jax.random.uniform(jax.random.fold_in(jax.random.fold_in(own_key, 6), dim), (shards_of,), jnp.float32, smallest / len(shards), high / len(shards))
        loudness = loudness * jnp.repeat(jnp.exp(heights), extent[dim] // shards_of).reshape((-1,) + (1,) * (len(extent) - 1 - dim))
    return loudness


def scatter_about(rng, dims, scale, reach, shards=(), kind=jnp.bfloat16):
    entries = jax.random.normal(rng, dims, jnp.float32) * scale
    if len(shards) > 0:
        entries = block_scale(rng, dims, shards, -0.22, 0.18) * entries
    return jnp.clip(entries, min=-reach, max=reach).astype(kind)


def setup_inputs(seed: int = 0) -> dict:
    streams_of = jax.random.split(jax.random.key(seed), 9)
    incoming = draw_incoming(jax.random.fold_in(streams_of[8], 71), 0)
    grad_in = scatter_about(streams_of[1], (SECTIONS, TOKENS, D), 1.0, 6.0, ((0, 16), (1, 16)))
    held = draw_held(jax.random.fold_in(streams_of[8], 71), 0)
    roster = with_ends(jax.random.randint(streams_of[3], (SECTIONS, 2), 0, SLOTS), jax.random.fold_in(streams_of[3], 1), 0, SLOTS - 1).astype(jnp.int32)
    norm_gain = jnp.clip(1.0 + 0.15 * jax.random.normal(streams_of[4], (SECTIONS, D), jnp.float32), 0.25, 1.75)
    r_scores = draw_r_scores(jax.random.fold_in(streams_of[8], 71), 0)
    value_weight = scatter_about(streams_of[6], (SECTIONS, D, HEADS * HEAD), D ** -0.5, 0.078125, ((0, 16), (2, 16)))
    out_weight = scatter_about(streams_of[7], (SECTIONS, HEADS * HEAD, D), (HEADS * HEAD) ** -0.5, 0.078125, ((0, 16), (1, 16)))
    return dict(incoming=incoming, grad_in=grad_in, held=held, roster=roster, norm_gain=norm_gain, r_scores=r_scores, value_weight=value_weight, out_weight=out_weight)


EPS = 0.5

def row_scale(values):
    return jnp.sqrt(lax.optimization_barrier(jnp.mean(values * values, axis=-1, keepdims=True)) + EPS)

def causal_probs(scores):
    length = scores.shape[-1]
    query_pos = jnp.arange(length)[:, None]
    key_pos = jnp.arange(length)[None, :]
    allowed = key_pos <= query_pos
    masked = jnp.where(allowed, scores, -jnp.inf)
    highest = lax.optimization_barrier(jnp.max(masked, axis=-1, keepdims=True))
    expo = jnp.where(allowed, jnp.exp(masked - highest), 0.0)
    return (expo / lax.optimization_barrier(jnp.sum(expo, axis=-1, keepdims=True))).astype(jnp.bfloat16)

def section_pass(operands):
    tokens_in, grad_rows, stash, gain, scores, w_value, w_out = operands
    length = tokens_in.shape[0]
    width = tokens_in.shape[1]
    heads = scores.shape[0]
    attn_probs = causal_probs(scores).astype(jnp.float32)
    tokens_f32 = tokens_in.astype(jnp.float32)
    normed = (tokens_f32 / row_scale(tokens_f32) * gain).astype(jnp.bfloat16)
    values = jnp.dot(normed, w_value, preferred_element_type=jnp.float32).astype(jnp.bfloat16)
    split_values = values.astype(jnp.float32).reshape(length, heads, -1)
    context = jnp.einsum('hij,jhd->ihd', attn_probs, split_values, precision=lax.Precision.HIGHEST)
    context = context.astype(jnp.bfloat16).reshape(length, -1)
    update = jnp.dot(context, w_out, preferred_element_type=jnp.float32)
    layer_out = (tokens_f32 + update).astype(jnp.bfloat16)
    grad_context = lax.dot_general(grad_rows, w_out, (((1,), (1,)), ((), ())), preferred_element_type=jnp.float32).astype(jnp.bfloat16)
    split_grad = grad_context.astype(jnp.float32).reshape(length, heads, -1)
    grad_values = jnp.einsum('hij,ihd->jhd', attn_probs, split_grad, precision=lax.Precision.HIGHEST)
    grad_values = grad_values.astype(jnp.bfloat16).reshape(length, -1)
    grad_normed = lax.dot_general(grad_values, w_value, (((1,), (1,)), ((), ())), preferred_element_type=jnp.float32)
    stash_f32 = stash.astype(jnp.float32)
    stash_scale = row_scale(stash_f32)
    inner_sum = lax.optimization_barrier(jnp.sum(gain * grad_normed * stash_f32, axis=-1, keepdims=True))
    input_grad = grad_rows.astype(jnp.float32) + gain * grad_normed / stash_scale - stash_f32 * inner_sum / (width * stash_scale ** 3)
    return (layer_out, input_grad.astype(jnp.bfloat16))

def reference(incoming, grad_in, held, roster, norm_gain, r_scores, value_weight, out_weight):
    count = incoming.shape[0]
    section_ids = jnp.arange(count).astype(jnp.int32)
    fetched = held[::-1][section_ids, roster[:, 0].astype(jnp.int32)]
    mirror_plan = roster[::-1]
    slot_ids = jnp.arange(held.shape[1]).astype(jnp.int32)
    chosen = slot_ids[None, :] == mirror_plan[:, 1][:, None]
    held_next = jnp.where(chosen[:, :, None, None], incoming[::-1][:, None], held)
    layer_out, input_grad = lax.map(section_pass, (incoming, grad_in, fetched, norm_gain, r_scores, value_weight, out_weight))
    return (jnp.roll(layer_out, 1, axis=0), jnp.roll(input_grad, -1, axis=0), held_next)
```

```python
import jax
import jax.numpy as jnp
from jax import lax
from jax.sharding import PartitionSpec as P

EPS = 0.5

CHIPS = [(0, 0), (0, 1), (1, 0), (1, 1), (2, 0), (2, 1), (3, 0), (3, 1)]
FAR_FIRST = [(2, 1), (2, 0), (1, 1), (3, 1), (1, 0), (3, 0), (0, 1)]


def moved(index, dx, dz):
    x, z, core = index // 4, index // 2 % 2, index % 2
    return (x + dx) % 4 * 4 + (z + dz) % 2 * 2 + core


def swap_cores(value):
    return lax.ppermute(value, "tp", [(i, i ^ 1) for i in range(16)])


def from_chip(value, dx, dz):
    return lax.ppermute(value, "tp", [(moved(i, dx, dz), i) for i in range(16)])


def to_chip(value, dx, dz):
    return lax.ppermute(value, "tp", [(i, moved(i, dx, dz)) for i in range(16)])


def row_scale(values):
    return jnp.sqrt(jnp.mean(values * values, axis=-1, keepdims=True) + EPS)


def causal_probs(scores):
    length = scores.shape[-1]
    query_pos = lax.broadcasted_iota(jnp.int32, (length, length), 0)
    key_pos = lax.broadcasted_iota(jnp.int32, (length, length), 1)
    allowed = key_pos <= query_pos
    masked = jnp.where(allowed, scores, -jnp.inf)
    highest = jnp.max(masked, axis=-1, keepdims=True)
    expo = jnp.where(allowed, jnp.exp(masked - highest), 0.0)
    return (expo / jnp.sum(expo, axis=-1, keepdims=True)).astype(jnp.bfloat16)


def in_core_order(core, own, other, axis):
    first = jnp.where(core == 0, own, other)
    second = jnp.where(core == 0, other, own)
    return jnp.concatenate([first, second], axis=axis)


def gather_rows(core, rows):
    half = rows.shape[1] // 2
    keep = lax.dynamic_slice_in_dim(rows, core * half, half, 1)
    give = lax.dynamic_slice_in_dim(rows, (1 - core) * half, half, 1)
    block = in_core_order(core, keep, swap_cores(give), 0)
    pieces = {(0, 0): block}
    for dx, dz in FAR_FIRST:
        pieces[dx, dz] = from_chip(block, dx, dz)
    return jnp.concatenate([pieces[chip] for chip in CHIPS], axis=0)


def scatter_rows(core, partial):
    block = partial.shape[0] // 8
    rounded = partial.astype(jnp.bfloat16)
    total = partial[:block]
    arrived = []
    for dx, dz in FAR_FIRST:
        at = CHIPS.index((dx, dz)) * block
        arrived.append(to_chip(rounded[at : at + block], dx, dz))
    for value in arrived:
        total = total + value.astype(jnp.float32)
    rows = block // 2
    keep = lax.dynamic_slice_in_dim(total, core * rows, rows, 0)
    give = lax.dynamic_slice_in_dim(total, (1 - core) * rows, rows, 0)
    return in_core_order(core, keep, swap_cores(give), 1)


def both_cores(partial):
    width = partial.shape[1] // 2
    other = swap_cores(partial)
    return partial + jnp.concatenate([other[:, width:], other[:, :width]], axis=1)


def body(incoming, grad_in, held, roster, norm_gain, r_scores, value_weight, out_weight):
    tokens_here = incoming[0]
    grad_here = grad_in[0]
    stash_store = held[0]
    gain = norm_gain[0]
    w_value = value_weight[0]
    w_out = out_weight[0]
    width = tokens_here.shape[1]
    half = width // 2
    tp = lax.axis_index("tp")
    core, z, x = tp % 2, tp // 2 % 2, tp // 4
    sections = lax.axis_size("section")
    ring = range(sections)

    grads = gather_rows(core, grad_here)
    tokens_f32 = tokens_here.astype(jnp.float32)
    normed_here = (tokens_f32 / row_scale(tokens_f32) * gain).astype(jnp.bfloat16)
    normed = gather_rows(core, normed_here)

    out_keep = lax.dynamic_slice_in_dim(w_out, core * half, half, 1)
    out_give = lax.dynamic_slice_in_dim(w_out, (1 - core) * half, half, 1)
    w_out_half = jnp.concatenate([out_keep, swap_cores(out_give)], axis=0)
    value_keep = lax.dynamic_slice_in_dim(w_value, core * half, half, 0)
    value_give = lax.dynamic_slice_in_dim(w_value, (1 - core) * half, half, 0)
    w_value_half = jnp.concatenate([value_keep, swap_cores(value_give)], axis=1)

    seq_len = r_scores.shape[2]
    position = lax.broadcasted_iota(jnp.int32, (seq_len, seq_len), 0)
    token = (x + position // 64) % 4 * 64 + (z + position // 32 % 2) % 2 * 32 + position % 32
    order = (token == lax.broadcasted_iota(jnp.int32, (seq_len, seq_len), 1)).astype(jnp.bfloat16)
    probs_here = causal_probs(r_scores[0])
    probs_here = jnp.einsum("qa,hab->hqb", order, probs_here)
    probs_here = jnp.einsum("hqb,kb->hqk", probs_here, order)
    probs = jnp.concatenate([probs_here, swap_cores(probs_here)], axis=0)
    heads = probs.shape[0]

    mirror = sections - 1 - lax.axis_index("section")
    mirror_plan = lax.dynamic_index_in_dim(roster, mirror, 0, keepdims=False)
    outgoing = lax.dynamic_index_in_dim(stash_store, mirror_plan[0], 0, keepdims=False)
    mirrored = [(s, sections - 1 - s) for s in ring]
    arriving = lax.ppermute(tokens_here, "section", mirrored)
    fetched = lax.ppermute(outgoing, "section", mirrored)
    slot_match = jnp.arange(stash_store.shape[0]) == mirror_plan[1]
    held_next = jnp.where(slot_match[:, None, None], arriving[None], stash_store)

    grad_context = lax.dot_general(
        grads, w_out_half, (((1,), (1,)), ((), ())), preferred_element_type=jnp.float32
    )
    grad_context = both_cores(grad_context).astype(jnp.bfloat16)
    grad_values = jnp.einsum(
        "hij,ihd->jhd",
        probs,
        grad_context.reshape(seq_len, heads, -1),
        preferred_element_type=jnp.float32,
    )
    grad_values = grad_values.astype(jnp.bfloat16).reshape(seq_len, -1)
    grad_normed = lax.dot_general(
        grad_values, w_value_half, (((1,), (1,)), ((), ())), preferred_element_type=jnp.float32
    )
    grad_normed = scatter_rows(core, grad_normed)

    values = jnp.dot(normed, w_value_half, preferred_element_type=jnp.float32)
    values = both_cores(values).astype(jnp.bfloat16)
    context = jnp.einsum(
        "hij,jhd->ihd",
        probs,
        values.reshape(seq_len, heads, -1),
        preferred_element_type=jnp.float32,
    )
    context = context.astype(jnp.bfloat16).reshape(seq_len, -1)
    update = jnp.dot(context, w_out_half, preferred_element_type=jnp.float32)
    update = scatter_rows(core, update)

    stash_f32 = fetched.astype(jnp.float32)
    stash_scale = row_scale(stash_f32)
    inner_sum = jnp.sum(gain * grad_normed * stash_f32, axis=-1, keepdims=True)
    input_grad = (
        grad_here.astype(jnp.float32)
        + gain * grad_normed / stash_scale
        - stash_f32 * inner_sum / (width * stash_scale**3)
    )
    returned = lax.ppermute(
        input_grad.astype(jnp.bfloat16), "section", [(s, (s - 1) % sections) for s in ring]
    )
    layer_out = (tokens_f32 + update).astype(jnp.bfloat16)
    passed_on = lax.ppermute(layer_out, "section", [(s, (s + 1) % sections) for s in ring])
    return (passed_on[None], returned[None], held_next[None])


def solution(mesh):
    in_specs = (
        P("section", "tp", None),
        P("section", "tp", None),
        P("section", None, "tp", None),
        P(),
        P("section", None),
        P("section", "tp", None, None),
        P("section", None, "tp"),
        P("section", "tp", None),
    )
    out_specs = (P("section", "tp", None), P("section", "tp", None), P("section", None, "tp", None))
    return jax.shard_map(body, mesh=mesh, in_specs=in_specs, out_specs=out_specs, check_vma=False)
```

```python
import functools

import jax
import jax.numpy as jnp
from jax import lax
from jax.experimental import pallas as pl
from jax.experimental.pallas import tpu as pltpu
from jax.sharding import PartitionSpec as P


EPS = 0.5

A, B, Z, CORE = 4, 12, 2, 1
PLACE = {A: 1, B: 2, Z: 4}
THIRDS = ((A, B, Z), (B, Z, A), (Z, A, B))
ROWS = 32


def trade(value, distance):
    return lax.ppermute(value, "tp", [(i, i ^ distance) for i in range(16)])


def place(order, first, second, third):
    return first * PLACE[order[0]] + second * PLACE[order[1]] + third * PLACE[order[2]]


def row_scale(values):
    return jnp.sqrt(jnp.mean(values * values, axis=-1, keepdims=True) + EPS)


def causal_probs(scores):
    length = scores.shape[-1]
    query_pos = lax.broadcasted_iota(jnp.int32, (length, length), 0)
    key_pos = lax.broadcasted_iota(jnp.int32, (length, length), 1)
    allowed = key_pos <= query_pos
    masked = jnp.where(allowed, scores, -jnp.inf)
    highest = jnp.max(masked, axis=-1, keepdims=True)
    expo = jnp.where(allowed, jnp.exp(masked - highest), 0.0)
    return (expo / jnp.sum(expo, axis=-1, keepdims=True)).astype(jnp.bfloat16)


def call(kernel, outs, args, scratch=(), core=None, mib=6):
    vmem = pl.BlockSpec(memory_space=pltpu.VMEM)
    in_specs = [vmem] * len(args)
    if core is not None:
        in_specs = [pl.BlockSpec(memory_space=pltpu.SMEM)] + in_specs
        args = [core] + list(args)
    return pl.pallas_call(
        kernel,
        out_shape=outs,
        in_specs=in_specs,
        out_specs=[vmem] * len(outs),
        scratch_shapes=list(scratch),
        compiler_params=pltpu.CompilerParams(vmem_limit_bytes=mib * 1024 * 1024),
    )(*args)


def dot(left, right, left_dim, right_dim):
    return lax.dot_general(
        left, right, (((left_dim,), (right_dim,)), ((), ())), preferred_element_type=jnp.float32
    )


def first_kernel(weight_dim, *refs):
    pieces, own, other, out, rows = refs[:6], refs[6], refs[7], refs[8], refs[9]
    third = rows.shape[1] // 3
    for t, order in enumerate(THIRDS):
        for late in range(2):
            for mid in range(2):
                for early in range(2):
                    to = place(order, early, mid, late) * ROWS
                    at = (mid * 2 + early) * ROWS
                    rows[to : to + ROWS, t * third : (t + 1) * third] = pieces[2 * t + late][at : at + ROWS, :]
    width = out.shape[1] // 2
    out[:, :width] = dot(rows[...], own[...], 1, weight_dim)
    out[:, width:] = dot(rows[...], other[...], 1, weight_dim)


def second_kernel(probs_dim, weight_dim, *refs):
    mine, theirs, probs, probs_other, own, other = refs[:6]
    outs, mixed = refs[6:12], refs[12]
    width = mine.shape[1] // 2
    head = 128
    for half, chances in enumerate((probs, probs_other)):
        for h in range(width // head):
            at = half * width + h * head
            across = (1 - half) * width + h * head
            whole = (mine[:, at : at + head] + theirs[:, across : across + head]).astype(jnp.bfloat16)
            mixed[:, at : at + head] = dot(chances[h], whole, probs_dim, 0).astype(jnp.bfloat16)
    third = outs[0].shape[1]
    step = 256
    for t, order in enumerate(THIRDS):
        send, keep = outs[2 * t], outs[2 * t + 1]
        for c in range(0, third, step):
            cols = slice(t * third + c, t * third + c + step)
            if weight_dim == 1:
                total = dot(mixed[:, :width], own[cols, :], 1, 1) + dot(mixed[:, width:], other[cols, :], 1, 1)
            else:
                total = dot(mixed[:, :width], own[:, cols], 1, 0) + dot(mixed[:, width:], other[:, cols], 1, 0)
            for mid in range(2):
                for late in range(2):
                    to = (mid * 2 + late) * ROWS
                    at = place(order, 0, mid, late) * ROWS
                    keep[to : to + ROWS, c : c + step] = total[at : at + ROWS]
                    at = place(order, 1, mid, late) * ROWS
                    send[to : to + ROWS, c : c + step] = total[at : at + ROWS].astype(jnp.bfloat16)


def add_kernel(*refs):
    ins, outs = refs[:6], refs[6:]
    for t in range(3):
        kept, came = ins[2 * t], ins[2 * t + 1]
        rows = kept.shape[0] // 2
        outs[2 * t + 1][...] = kept[:rows] + came[:rows].astype(jnp.float32)
        outs[2 * t][...] = (kept[rows:] + came[rows:].astype(jnp.float32)).astype(jnp.bfloat16)


def last_add_kernel(*refs):
    core, ins, outs = refs[0], refs[1:7], refs[7:]
    third = ins[0].shape[1]
    rows = ROWS // 2
    stay = pl.multiple_of(core[0] * rows, rows)
    go = pl.multiple_of((1 - core[0]) * rows, rows)
    for t in range(3):
        kept, came = ins[2 * t], ins[2 * t + 1]
        cols = slice(t * third, (t + 1) * third)
        for out, at in ((outs[0], go), (outs[1], stay)):
            out[:, cols] = kept[pl.ds(at, rows), :] + came[pl.ds(at, rows), :].astype(jnp.float32)


def split_kernel(core, rows, go, stay):
    half = go.shape[1]
    lower = core[0] == 0
    go[...] = jnp.where(lower, rows[:, half:], rows[:, :half])
    stay[...] = jnp.where(lower, rows[:, :half], rows[:, half:])


def norm_kernel(core, rows, gain, go, stay):
    half = go.shape[1]
    values = rows[...].astype(jnp.float32)
    normed = (values / row_scale(values) * gain[...]).astype(jnp.bfloat16)
    lower = core[0] == 0
    go[...] = jnp.where(lower, normed[:, half:], normed[:, :half])
    stay[...] = jnp.where(lower, normed[:, :half], normed[:, half:])


def block_kernel(core, stay, came, *outs):
    rows, third = stay.shape[0], outs[0].shape[1]
    lower = core[0] == 0
    for t, out in enumerate(outs):
        cols = slice(t * third, (t + 1) * third)
        out[:rows] = jnp.where(lower, stay[:, cols], came[:, cols])
        out[rows:] = jnp.where(lower, came[:, cols], stay[:, cols])


def join_kernel(*refs):
    for t in range(3):
        had, came, out = refs[2 * t], refs[2 * t + 1], refs[6 + t]
        rows = had.shape[0]
        out[:rows] = had[...]
        out[rows:] = came[...]


def whole(core, stay, came):
    lower = core[0] == 0
    return jnp.concatenate(
        [jnp.where(lower, stay[...], came[...]), jnp.where(lower, came[...], stay[...])], axis=1
    )


def end_f_kernel(core, stay, came, tokens, out):
    out[...] = (tokens[...].astype(jnp.float32) + whole(core, stay, came)).astype(jnp.bfloat16)


def end_b_kernel(core, stay, came, grads, stash, gain, out):
    weighted = gain[...] * whole(core, stay, came)
    stash_f32 = stash[...].astype(jnp.float32)
    scale = row_scale(stash_f32)
    inner_sum = jnp.sum(weighted * stash_f32, axis=-1, keepdims=True)
    width = stash_f32.shape[1]
    out[...] = (
        grads[...].astype(jnp.float32) + weighted / scale - stash_f32 * inner_sum / (width * (scale * scale * scale))
    ).astype(jnp.bfloat16)


def gather_stage(stage, held):
    return [trade(held[t], THIRDS[t][stage]) for t in range(3)]


def scatter_stage(stage, sends):
    return [trade(sends[t], THIRDS[t][stage]) for t in range(3)]


def body(incoming, grad_in, held, roster, norm_gain, r_scores, value_weight, out_weight):
    tokens_here = incoming[0]
    grad_here = grad_in[0]
    stash_store = held[0]
    gain = norm_gain[0]
    w_value = value_weight[0]
    w_out = out_weight[0]
    width = tokens_here.shape[1]
    half = width // 2
    third = half // 3
    bf16, f32 = jnp.bfloat16, jnp.float32
    tp = lax.axis_index("tp")
    core, z, x = tp % 2, tp // 2 % 2, tp // 4
    sections = lax.axis_size("section")
    ring = range(sections)
    shape = jax.ShapeDtypeStruct

    core_index = core[None].astype(jnp.int32)
    halved = [shape((ROWS // 2, half), bf16)] * 2

    def block(go, stay):
        came = trade(go, CORE)
        return call(block_kernel, [shape((ROWS, third), bf16)] * 3, [stay, came], core=core_index)

    grads = block(*call(split_kernel, halved, [grad_here], core=core_index))
    normed = block(*call(norm_kernel, halved, [tokens_here, gain[None]], core=core_index))

    def pieces(rows, came):
        return [piece for pair in zip(rows, came) for piece in pair]

    def stage(s, rows, came):
        if came is not None:
            joined = [shape((2 * rows[0].shape[0], third), bf16)] * 3
            rows = call(join_kernel, joined, pieces(rows, came))
        return rows, gather_stage(s, rows)

    grads, grads_came = stage(0, grads, None)
    normed, normed_came = stage(0, normed, None)
    grads, grads_came = stage(1, grads, grads_came)
    normed, normed_came = stage(1, normed, normed_came)
    grads, grads_came = stage(2, grads, grads_came)
    normed, normed_came = stage(2, normed, normed_came)

    out_own = lax.dynamic_slice_in_dim(w_out, core * half, half, 1)
    out_other = trade(lax.dynamic_slice_in_dim(w_out, (1 - core) * half, half, 1), CORE)
    value_own = lax.dynamic_slice_in_dim(w_value, core * half, half, 0)
    value_other = trade(lax.dynamic_slice_in_dim(w_value, (1 - core) * half, half, 0), CORE)

    seq_len = r_scores.shape[2]
    position = lax.broadcasted_iota(jnp.int32, (seq_len, seq_len), 0)
    at = position // ROWS
    token = ((x ^ at % 2 ^ at // 2 % 2 * 3) * 2 + (z ^ at // 4)) * ROWS + position % ROWS
    order = (token == lax.broadcasted_iota(jnp.int32, (seq_len, seq_len), 1)).astype(bf16)
    probs = causal_probs(r_scores[0])
    probs = jnp.einsum("qa,hab->hqb", order, probs)
    probs = jnp.einsum("hqb,kb->hqk", probs, order)
    probs_other = trade(probs, CORE)

    mirror = sections - 1 - lax.axis_index("section")
    mirror_plan = lax.dynamic_index_in_dim(roster, mirror, 0, keepdims=False)
    outgoing = lax.dynamic_index_in_dim(stash_store, mirror_plan[0], 0, keepdims=False)
    mirrored = [(s, sections - 1 - s) for s in ring]
    arriving = lax.ppermute(tokens_here, "section", mirrored)
    fetched = lax.ppermute(outgoing, "section", mirrored)
    slot_match = jnp.arange(stash_store.shape[0]) == mirror_plan[1]
    held_next = jnp.where(slot_match[:, None, None], arriving[None], stash_store)

    heads_width = w_out.shape[0]
    partial = [shape((seq_len, 2 * heads_width), f32)]
    rows_scratch = [pltpu.VMEM((seq_len, half), bf16)]
    split = [shape((seq_len // 2, third), t) for _ in range(3) for t in (bf16, f32)]
    mixed_scratch = [pltpu.VMEM((seq_len, 2 * heads_width), bf16)]

    def halves(rows):
        return [shape((rows, third), t) for _ in range(3) for t in (bf16, f32)]

    def first(rows, came, own, other, weight_dim):
        return call(
            functools.partial(first_kernel, weight_dim), partial, pieces(rows, came) + [own, other], rows_scratch,
            mib=14,
        )[0]

    def second(mine, theirs, own, other, probs_dim, weight_dim):
        return call(
            functools.partial(second_kernel, probs_dim, weight_dim),
            split, [mine, theirs, probs, probs_other, own, other], mixed_scratch, mib=18,
        )

    def add(parts, came, rows):
        return call(add_kernel, halves(rows), pieces(parts[1::2], came))

    def last_add(parts, came):
        outs = [shape((ROWS // 2, half), f32)] * 2
        return call(last_add_kernel, outs, pieces(parts[1::2], came), core=core_index)

    mine_b = first(grads, grads_came, out_own, out_other, 1)
    theirs_b = trade(mine_b, CORE)
    parts_b = second(mine_b, theirs_b, value_own, value_other, 0, 1)
    mine_f = first(normed, normed_came, value_own, value_other, 0)
    theirs_f = trade(mine_f, CORE)
    parts_f = second(mine_f, theirs_f, out_own, out_other, 1, 0)

    came_b = scatter_stage(0, parts_b[0::2])
    came_f = scatter_stage(0, parts_f[0::2])
    parts_b = add(parts_b, came_b, 64)
    came_b = scatter_stage(1, parts_b[0::2])
    parts_f = add(parts_f, came_f, 64)
    came_f = scatter_stage(1, parts_f[0::2])
    parts_b = add(parts_b, came_b, 32)
    came_b = scatter_stage(2, parts_b[0::2])
    parts_f = add(parts_f, came_f, 32)
    came_f = scatter_stage(2, parts_f[0::2])
    go_b, stay_b = last_add(parts_b, came_b)
    go_f, stay_f = last_add(parts_f, came_f)
    ended = [shape(tokens_here.shape, bf16)]
    end_b = [stay_b, trade(go_b, CORE), grad_here, fetched, gain[None]]
    input_grad = call(end_b_kernel, ended, end_b, core=core_index)[0]
    end_f = [stay_f, trade(go_f, CORE), tokens_here]
    layer_out = call(end_f_kernel, ended, end_f, core=core_index)[0]
    returned = lax.ppermute(input_grad, "section", [(s, (s - 1) % sections) for s in ring])
    passed_on = lax.ppermute(layer_out, "section", [(s, (s + 1) % sections) for s in ring])
    return (passed_on[None], returned[None], held_next[None])


def solution(mesh):
    in_specs = (
        P("section", "tp", None),
        P("section", "tp", None),
        P("section", None, "tp", None),
        P(),
        P("section", None),
        P("section", "tp", None, None),
        P("section", None, "tp"),
        P("section", "tp", None),
    )
    out_specs = (P("section", "tp", None), P("section", "tp", None), P("section", None, "tp", None))

    return jax.shard_map(body, mesh=mesh, in_specs=in_specs, out_specs=out_specs, check_vma=False)
```

```python
import functools

import jax
import jax.numpy as jnp
from jax import lax
from jax.experimental import pallas as pl
from jax.experimental.pallas import tpu as pltpu
from jax.sharding import PartitionSpec as P


EPS = 0.5

A, B, Z, CORE = 4, 12, 2, 1
PLACE = {A: 1, B: 2, Z: 4}
GATHERS = ((Z, A, B), (Z, B, A))
SCATTERS = ((A, B, Z), (B, A, Z))
ROWS = 32


def trade(value, distance):
    return lax.ppermute(value, "tp", [(i, i ^ distance) for i in range(16)])


def place(order, first, second, third):
    return first * PLACE[order[0]] + second * PLACE[order[1]] + third * PLACE[order[2]]


def row_scale(values):
    return jnp.sqrt(jnp.mean(values * values, axis=-1, keepdims=True) + EPS)


def call(kernel, outs, args, scratch=(), smem=0, mib=6):
    vmem = pl.BlockSpec(memory_space=pltpu.VMEM)
    in_specs = [pl.BlockSpec(memory_space=pltpu.SMEM)] * smem + [vmem] * (len(args) - smem)
    return pl.pallas_call(
        kernel,
        out_shape=outs,
        in_specs=in_specs,
        out_specs=[vmem] * len(outs),
        scratch_shapes=list(scratch),
        compiler_params=pltpu.CompilerParams(vmem_limit_bytes=mib * 1024 * 1024),
    )(*args)


def core_here():
    return lax.axis_index("tp") & 1


def dot(left, right, left_dim, right_dim):
    return lax.dot_general(
        left, right, (((left_dim,), (right_dim,)), ((), ())), preferred_element_type=jnp.float32
    )


def columns(start, size):
    return pl.ds(pl.multiple_of(start, 128), size)


def fill(pieces, rows):
    part = rows.shape[1] // 2
    for t, order in enumerate(GATHERS):
        for late in range(2):
            for mid in range(2):
                for early in range(2):
                    to = place(order, early, mid, late) * ROWS
                    at = (mid * 2 + early) * ROWS
                    rows[to : to + ROWS, t * part : (t + 1) * part] = pieces[2 * t + late][at : at + ROWS, :]


def first_b_kernel(*refs):
    pieces, own, other, out, rows = refs[:4], refs[4], refs[5], refs[6], refs[7]
    fill(pieces, rows)
    half, heads = rows.shape[1], own.shape[0]
    out[:, :heads] = dot(rows[...], own[:, columns(core_here() * half, half)], 1, 1)
    out[:, heads:] = dot(rows[...], other[...], 1, 1)


def first_f_kernel(*refs):
    pieces, own, other, out, rows = refs[:4], refs[4], refs[5], refs[6], refs[7]
    fill(pieces, rows)
    half, heads = rows.shape[1], own.shape[1]
    out[:, :heads] = dot(rows[...], own[columns(core_here() * half, half), :], 1, 0)
    out[:, heads:] = dot(rows[...], other[...], 1, 0)


def second_kernel(probs_dim, weight_dim, *refs):
    mine, theirs, probs, probs_other, own, other = refs[:6]
    outs, mixed = refs[6:10], refs[10]
    width = mine.shape[1] // 2
    head = 128
    for half, chances in enumerate((probs, probs_other)):
        for h in range(width // head):
            at = half * width + h * head
            across = (1 - half) * width + h * head
            whole = (mine[:, at : at + head] + theirs[:, across : across + head]).astype(jnp.bfloat16)
            mixed[:, at : at + head] = dot(chances[h], whole, probs_dim, 0).astype(jnp.bfloat16)
    part = outs[0].shape[1]
    step = 256
    start = core_here() * (2 * part)
    for t, order in enumerate(SCATTERS):
        send, keep = outs[2 * t], outs[2 * t + 1]
        for c in range(0, part, step):
            cols = slice(t * part + c, t * part + c + step)
            own_cols = columns(start + cols.start, step)
            if weight_dim == 1:
                total = dot(mixed[:, :width], own[own_cols, :], 1, 1) + dot(mixed[:, width:], other[cols, :], 1, 1)
            else:
                total = dot(mixed[:, :width], own[:, own_cols], 1, 0) + dot(mixed[:, width:], other[:, cols], 1, 0)
            for mid in range(2):
                for late in range(2):
                    to = (mid * 2 + late) * ROWS
                    at = place(order, 0, mid, late) * ROWS
                    keep[to : to + ROWS, c : c + step] = total[at : at + ROWS]
                    at = place(order, 1, mid, late) * ROWS
                    send[to : to + ROWS, c : c + step] = total[at : at + ROWS].astype(jnp.bfloat16)


def add_kernel(*refs):
    ins, outs = refs[:4], refs[4:]
    for t in range(2):
        kept, came = ins[2 * t], ins[2 * t + 1]
        rows = kept.shape[0] // 2
        if len(outs) == 2:
            send = outs[0].at[:, t * kept.shape[1] : (t + 1) * kept.shape[1]]
            keep = outs[1].at[:, t * kept.shape[1] : (t + 1) * kept.shape[1]]
        else:
            send, keep = outs[2 * t], outs[2 * t + 1]
        keep[...] = kept[:rows] + came[:rows].astype(jnp.float32)
        send[...] = (kept[rows:] + came[rows:].astype(jnp.float32)).astype(jnp.bfloat16)


def last_add_kernel(kept, came, go, stay):
    rows = ROWS // 2
    core = core_here()
    for out, which in ((go, 1 - core), (stay, core)):
        at = pl.multiple_of(which * rows, rows)
        out[...] = kept[pl.ds(at, rows), :] + came[pl.ds(at, rows), :].astype(jnp.float32)


def split_kernel(rows, go, stay):
    half = go.shape[1]
    lower = core_here() == 0
    go[...] = jnp.where(lower, rows[:, half:], rows[:, :half])
    stay[...] = jnp.where(lower, rows[:, :half], rows[:, half:])


def norm_kernel(rows, gain, go, stay):
    half = go.shape[1]
    values = rows[...].astype(jnp.float32)
    normed = (values / row_scale(values) * gain[...]).astype(jnp.bfloat16)
    lower = core_here() == 0
    go[...] = jnp.where(lower, normed[:, half:], normed[:, :half])
    stay[...] = jnp.where(lower, normed[:, :half], normed[:, half:])


def block_kernel(stay, came, out):
    rows = stay.shape[0]
    lower = core_here() == 0
    out[:rows] = jnp.where(lower, stay[...], came[...])
    out[rows:] = jnp.where(lower, came[...], stay[...])


def first_join_kernel(had, came, *outs):
    rows, part = had.shape[0], outs[0].shape[1]
    for t, out in enumerate(outs):
        out[:rows] = had[:, t * part : (t + 1) * part]
        out[rows:] = came[:, t * part : (t + 1) * part]


def join_kernel(*refs):
    for t in range(2):
        had, came, out = refs[2 * t], refs[2 * t + 1], refs[4 + t]
        rows = had.shape[0]
        out[:rows] = had[...]
        out[rows:] = came[...]


def whole(stay, came):
    lower = core_here() == 0
    return jnp.concatenate(
        [jnp.where(lower, stay[...], came[...]), jnp.where(lower, came[...], stay[...])], axis=1
    )


def end_f_kernel(stay, came, tokens, out):
    out[...] = (tokens[...].astype(jnp.float32) + whole(stay, came)).astype(jnp.bfloat16)


def end_b_kernel(stay, came, grads, stash, gain, out):
    weighted = gain[...] * whole(stay, came)
    stash_f32 = stash[...].astype(jnp.float32)
    scale = row_scale(stash_f32)
    inner_sum = jnp.sum(weighted * stash_f32, axis=-1, keepdims=True)
    width = stash_f32.shape[1]
    out[...] = (
        grads[...].astype(jnp.float32) + weighted / scale - stash_f32 * inner_sum / (width * (scale * scale * scale))
    ).astype(jnp.bfloat16)


def give_out_kernel(weights, out):
    half = out.shape[1]
    out[...] = weights[:, columns((1 - core_here()) * half, half)]


def give_value_kernel(weights, out):
    half = out.shape[0]
    out[...] = weights[columns((1 - core_here()) * half, half), :]


def probs_kernel(scores, out):
    length = scores.shape[1]
    row = lax.broadcasted_iota(jnp.int32, (length, length), 0)
    col = lax.broadcasted_iota(jnp.int32, (length, length), 1)
    tp = lax.axis_index("tp")
    at = row >> 5
    token = (((tp >> 2) ^ (at & 1) ^ (((at >> 1) & 1) * 3)) << 6) | ((((tp >> 1) & 1) ^ (at >> 2)) << 5) | (row & 31)
    order = (token == col).astype(jnp.bfloat16)
    allowed = col <= row
    for h in range(scores.shape[0]):
        masked = jnp.where(allowed, scores[h], -jnp.inf)
        highest = jnp.max(masked, axis=-1, keepdims=True)
        expo = jnp.exp(masked - highest)
        probs = (expo / jnp.sum(expo, axis=-1, keepdims=True)).astype(jnp.bfloat16)
        probs = dot(order, probs, 1, 0).astype(jnp.bfloat16)
        out[h] = dot(probs, order, 1, 1).astype(jnp.bfloat16)


def stash_kernel(roster, store, out):
    out[...] = store[roster[0, 15 - lax.axis_index("section")]]


def held_kernel(roster, store, came, out):
    slot = roster[1, 15 - lax.axis_index("section")]
    for i in range(store.shape[0]):
        out[i] = jnp.where(slot == i, came[...], store[i])


def part_trades(distances, values):
    return [trade(value, distance) for value, distance in zip(values, distances)]


def body(incoming, grad_in, held, roster, norm_gain, r_scores, value_weight, out_weight):
    tokens_here = incoming[0]
    grad_here = grad_in[0]
    stash_store = held[0]
    gain = norm_gain[0]
    w_value = value_weight[0]
    w_out = out_weight[0]
    width = tokens_here.shape[1]
    half = width // 2
    part = half // 2
    bf16, f32 = jnp.bfloat16, jnp.float32
    sections = lax.axis_size("section")
    ring = range(sections)
    shape = jax.ShapeDtypeStruct

    halved = [shape((ROWS // 2, half), bf16)] * 2

    def pieces(rows, came):
        return [piece for pair in zip(rows, came) for piece in pair]

    def gather(go, stay):
        came = trade(go, CORE)
        rows = call(block_kernel, [shape((ROWS, half), bf16)], [stay, came])[0]
        came = trade(rows, Z)
        rows = call(first_join_kernel, [shape((2 * ROWS, part), bf16)] * 2, [rows, came])
        came = part_trades((A, B), rows)
        rows = call(join_kernel, [shape((4 * ROWS, part), bf16)] * 2, pieces(rows, came))
        return rows, part_trades((B, A), rows)

    grads, grads_came = gather(*call(split_kernel, halved, [grad_here]))
    normed, normed_came = gather(*call(norm_kernel, halved, [tokens_here, gain[None]]))

    heads_width = w_out.shape[0]
    out_give = call(give_out_kernel, [shape((heads_width, half), bf16)], [w_out], mib=9)[0]
    out_other = trade(out_give, CORE)
    value_give = call(give_value_kernel, [shape((half, heads_width), bf16)], [w_value], mib=9)[0]
    value_other = trade(value_give, CORE)

    seq_len = r_scores.shape[2]
    probs = call(probs_kernel, [shape(r_scores.shape[1:], bf16)], [r_scores[0]])[0]
    probs_other = trade(probs, CORE)

    outgoing = call(stash_kernel, [shape(tokens_here.shape, bf16)], [roster.T, stash_store], smem=1)[0]
    mirrored = [(s, sections - 1 - s) for s in ring]
    arriving = lax.ppermute(tokens_here, "section", mirrored)
    fetched = lax.ppermute(outgoing, "section", mirrored)
    held_next = call(held_kernel, [shape(stash_store.shape, bf16)], [roster.T, stash_store, arriving], smem=1)[0]

    partial = [shape((seq_len, 2 * heads_width), f32)]
    rows_scratch = [pltpu.VMEM((seq_len, half), bf16)]
    split = [shape((seq_len // 2, part), t) for _ in range(2) for t in (bf16, f32)]
    mixed_scratch = [pltpu.VMEM((seq_len, 2 * heads_width), bf16)]

    def first(kernel, rows, came, own, other):
        return call(kernel, partial, pieces(rows, came) + [own, other], rows_scratch, mib=16)[0]

    def second(mine, theirs, own, other, probs_dim, weight_dim):
        return call(
            functools.partial(second_kernel, probs_dim, weight_dim),
            split, [mine, theirs, probs, probs_other, own, other], mixed_scratch, mib=20,
        )

    def scatter(parts):
        came = part_trades((A, B), parts[0::2])
        sums = [shape((2 * ROWS, part), t) for _ in range(2) for t in (bf16, f32)]
        parts = call(add_kernel, sums, pieces(parts[1::2], came))
        came = part_trades((B, A), parts[0::2])
        sums = [shape((ROWS, half), t) for t in (bf16, f32)]
        send, keep = call(add_kernel, sums, pieces(parts[1::2], came))
        came = trade(send, Z)
        outs = [shape((ROWS // 2, half), f32)] * 2
        go, stay = call(last_add_kernel, outs, [keep, came])
        return stay, trade(go, CORE)

    mine_b = first(first_b_kernel, grads, grads_came, w_out, out_other)
    theirs_b = trade(mine_b, CORE)
    parts_b = second(mine_b, theirs_b, w_value, value_other, 0, 1)
    mine_f = first(first_f_kernel, normed, normed_came, w_value, value_other)
    theirs_f = trade(mine_f, CORE)
    parts_f = second(mine_f, theirs_f, w_out, out_other, 1, 0)

    ended = [shape(tokens_here.shape, bf16)]
    input_grad = call(end_b_kernel, ended, [*scatter(parts_b), grad_here, fetched, gain[None]])[0]
    layer_out = call(end_f_kernel, ended, [*scatter(parts_f), tokens_here])[0]
    returned = lax.ppermute(input_grad, "section", [(s, (s - 1) % sections) for s in ring])
    passed_on = lax.ppermute(layer_out, "section", [(s, (s + 1) % sections) for s in ring])
    return (passed_on[None], returned[None], held_next[None])


def solution(mesh):
    in_specs = (
        P("section", "tp", None),
        P("section", "tp", None),
        P("section", None, "tp", None),
        P(),
        P("section", None),
        P("section", "tp", None, None),
        P("section", None, "tp"),
        P("section", "tp", None),
    )
    out_specs = (P("section", "tp", None), P("section", "tp", None), P("section", None, "tp", None))

    return jax.shard_map(body, mesh=mesh, in_specs=in_specs, out_specs=out_specs, check_vma=False)
```

```python
import functools

import jax
import jax.numpy as jnp
from jax import lax
from jax.experimental import pallas as pl
from jax.experimental.pallas import tpu as pltpu
from jax.sharding import PartitionSpec as P


EPS = 0.5

A, B, Z, CORE = 4, 12, 2, 1
PLACE = {A: 1, B: 2, Z: 4}
HALVES = ((A, B), (B, A))
ROWS = 32


def trade(value, distance):
    return lax.ppermute(value, "tp", [(i, i ^ distance) for i in range(16)])


def place(order, first, second):
    return first * PLACE[order[0]] + second * PLACE[order[1]]


def row_scale(values):
    return jnp.sqrt(jnp.mean(values * values, axis=-1, keepdims=True) + EPS)


def call(kernel, outs, args, scratch=(), smem=0, mib=6):
    vmem = pl.BlockSpec(memory_space=pltpu.VMEM)
    in_specs = [pl.BlockSpec(memory_space=pltpu.SMEM)] * smem + [vmem] * (len(args) - smem)
    return pl.pallas_call(
        kernel,
        out_shape=outs,
        in_specs=in_specs,
        out_specs=[vmem] * len(outs),
        scratch_shapes=list(scratch),
        compiler_params=pltpu.CompilerParams(vmem_limit_bytes=mib * 1024 * 1024),
    )(*args)


def core_here():
    return lax.axis_index("tp") & 1


def dot(left, right, left_dim, right_dim):
    return lax.dot_general(
        left, right, (((left_dim,), (right_dim,)), ((), ())), preferred_element_type=jnp.float32
    )


def columns(start, size):
    return pl.ds(pl.multiple_of(start, 128), size)


def fill(z_first, pieces, rows):
    part = rows.shape[1] // 2
    for t, order in enumerate(HALVES):
        for late in range(2):
            for mid in range(2):
                for early in range(2):
                    first, z = (mid, early) if z_first else (early, mid)
                    to = (place(order, first, late) + z * PLACE[Z]) * ROWS
                    at = (mid * 2 + early) * ROWS
                    rows[to : to + ROWS, t * part : (t + 1) * part] = pieces[2 * t + late][at : at + ROWS, :]


def first_b_kernel(*refs):
    pieces, own, other, out, rows = refs[:4], refs[4], refs[5], refs[6], refs[7]
    fill(True, pieces, rows)
    half, heads = rows.shape[1], own.shape[0]
    out[:, :heads] = dot(rows[...], own[:, columns(core_here() * half, half)], 1, 1)
    out[:, heads:] = dot(rows[...], other[...], 1, 1)


def first_f_kernel(*refs):
    pieces, own, other, out, rows = refs[:4], refs[4], refs[5], refs[6], refs[7]
    fill(False, pieces, rows)
    half, heads = rows.shape[1], own.shape[1]
    out[:, :heads] = dot(rows[...], own[columns(core_here() * half, half), :], 1, 0)
    out[:, heads:] = dot(rows[...], other[...], 1, 0)


def mix(probs_dim, mine, theirs, probs, probs_other, mixed):
    width = mine.shape[1] // 2
    head = 128
    for half, chances in enumerate((probs, probs_other)):
        for h in range(width // head):
            at = half * width + h * head
            across = (1 - half) * width + h * head
            whole = (mine[:, at : at + head] + theirs[:, across : across + head]).astype(jnp.bfloat16)
            mixed[:, at : at + head] = dot(chances[h], whole, probs_dim, 0).astype(jnp.bfloat16)


STEP = 256


def second_kernel(bwd, mine, theirs, probs, probs_other, own, other, *refs):
    outs, mixed = refs[:4], refs[4]
    mix(0 if bwd else 1, mine, theirs, probs, probs_other, mixed)
    heads, part = other.shape[1 if bwd else 0], outs[0].shape[1]
    start = core_here() * (2 * part)
    for t, order in enumerate(HALVES):
        send, keep = outs[2 * t], outs[2 * t + 1]
        for c in range(0, part, STEP):
            at = t * part + c
            if bwd:
                total = dot(mixed[:, :heads], own[columns(start + at, STEP), :], 1, 1)
                total = total + dot(mixed[:, heads:], other[at : at + STEP, :], 1, 1)
            else:
                total = dot(mixed[:, :heads], own[:, columns(start + at, STEP)], 1, 0)
                total = total + dot(mixed[:, heads:], other[:, at : at + STEP], 1, 0)
            for mid in range(2):
                for late in range(2):
                    z, second = (mid, late) if bwd else (late, mid)
                    to = (mid * 2 + late) * ROWS
                    row = (place(order, 0, second) + z * PLACE[Z]) * ROWS
                    keep[to : to + ROWS, c : c + STEP] = total[row : row + ROWS]
                    row = (place(order, 1, second) + z * PLACE[Z]) * ROWS
                    send[to : to + ROWS, c : c + STEP] = total[row : row + ROWS].astype(jnp.bfloat16)


def add_z_kernel(kept, came, *outs):
    part = outs[0].shape[1]
    for t in range(2):
        cols = slice(t * part, (t + 1) * part)
        total = kept[:, cols] + came[:, cols].astype(jnp.float32)
        outs[2 * t][...] = total[ROWS:].astype(jnp.bfloat16)
        outs[2 * t + 1][...] = total[:ROWS]


def add_kernel(*refs):
    ins, outs = refs[:4], refs[4:]
    for t in range(2):
        kept, came = ins[2 * t], ins[2 * t + 1]
        rows = kept.shape[0] // 2
        if len(outs) == 2:
            send = outs[0].at[:, t * kept.shape[1] : (t + 1) * kept.shape[1]]
            keep = outs[1].at[:, t * kept.shape[1] : (t + 1) * kept.shape[1]]
        else:
            send, keep = outs[2 * t], outs[2 * t + 1]
        keep[...] = kept[:rows] + came[:rows].astype(jnp.float32)
        send[...] = (kept[rows:] + came[rows:].astype(jnp.float32)).astype(jnp.bfloat16)


def last_add_b_kernel(*refs):
    ins, go, stay = refs[:4], refs[4], refs[5]
    rows = ROWS // 2
    core = core_here()
    for t in range(2):
        kept, came = ins[2 * t], ins[2 * t + 1]
        part = kept.shape[1]
        for out, which in ((go, 1 - core), (stay, core)):
            at = pl.multiple_of(which * rows, rows)
            sums = kept[pl.ds(at, rows), :] + came[pl.ds(at, rows), :].astype(jnp.float32)
            out[:, t * part : (t + 1) * part] = sums


def last_add_f_kernel(kept, came, go, stay):
    rows = ROWS // 2
    core = core_here()
    for out, which in ((go, 1 - core), (stay, core)):
        at = pl.multiple_of(which * rows, rows)
        out[...] = kept[pl.ds(at, rows), :] + came[pl.ds(at, rows), :].astype(jnp.float32)


def split_kernel(rows, go, stay):
    half = go.shape[1]
    lower = core_here() == 0
    go[...] = jnp.where(lower, rows[:, half:], rows[:, :half])
    stay[...] = jnp.where(lower, rows[:, :half], rows[:, half:])


def norm_kernel(rows, gain, go, stay):
    half = go.shape[1]
    values = rows[...].astype(jnp.float32)
    normed = (values / row_scale(values) * gain[...]).astype(jnp.bfloat16)
    lower = core_here() == 0
    go[...] = jnp.where(lower, normed[:, half:], normed[:, :half])
    stay[...] = jnp.where(lower, normed[:, :half], normed[:, half:])


def block_kernel(stay, came, *outs):
    rows, part = stay.shape[0], outs[0].shape[1]
    lower = core_here() == 0
    for t, out in enumerate(outs):
        mine, other = stay[:, t * part : (t + 1) * part], came[:, t * part : (t + 1) * part]
        out[:rows] = jnp.where(lower, mine, other)
        out[rows:] = jnp.where(lower, other, mine)


def split_join_kernel(had, came, *outs):
    rows, part = had.shape[0], outs[0].shape[1]
    for t, out in enumerate(outs):
        out[:rows] = had[:, t * part : (t + 1) * part]
        out[rows:] = came[:, t * part : (t + 1) * part]


def join_kernel(*refs):
    ins, outs = refs[:4], refs[4:]
    for t in range(2):
        had, came = ins[2 * t], ins[2 * t + 1]
        rows, part = had.shape
        out = outs[t] if len(outs) == 2 else outs[0].at[:, t * part : (t + 1) * part]
        out[:rows] = had[...]
        out[rows:] = came[...]


def copy_kernel(value, out):
    out[...] = value[...]


def whole(stay, came):
    lower = core_here() == 0
    return jnp.concatenate(
        [jnp.where(lower, stay[...], came[...]), jnp.where(lower, came[...], stay[...])], axis=1
    )


def end_f_kernel(stay, came, tokens, out):
    out[...] = (tokens[...].astype(jnp.float32) + whole(stay, came)).astype(jnp.bfloat16)


def end_b_kernel(stay, came, grads, stash, gain, out):
    weighted = gain[...] * whole(stay, came)
    stash_f32 = stash[...].astype(jnp.float32)
    scale = row_scale(stash_f32)
    inner_sum = jnp.sum(weighted * stash_f32, axis=-1, keepdims=True)
    width = stash_f32.shape[1]
    out[...] = (
        grads[...].astype(jnp.float32) + weighted / scale - stash_f32 * inner_sum / (width * (scale * scale * scale))
    ).astype(jnp.bfloat16)


def give_out_kernel(weights, out):
    half = out.shape[1]
    out[...] = weights[:, columns((1 - core_here()) * half, half)]


def give_value_kernel(weights, out):
    half = out.shape[0]
    out[...] = weights[columns((1 - core_here()) * half, half), :]


def probs_kernel(scores, out):
    length = scores.shape[1]
    row = lax.broadcasted_iota(jnp.int32, (length, length), 0)
    col = lax.broadcasted_iota(jnp.int32, (length, length), 1)
    tp = lax.axis_index("tp")
    at = row >> 5
    token = (((tp >> 2) ^ (at & 1) ^ (((at >> 1) & 1) * 3)) << 6) | ((((tp >> 1) & 1) ^ (at >> 2)) << 5) | (row & 31)
    order = (token == col).astype(jnp.bfloat16)
    allowed = col <= row
    for h in range(scores.shape[0]):
        masked = jnp.where(allowed, scores[h], -jnp.inf)
        highest = jnp.max(masked, axis=-1, keepdims=True)
        expo = jnp.exp(masked - highest)
        probs = (expo / jnp.sum(expo, axis=-1, keepdims=True)).astype(jnp.bfloat16)
        probs = dot(order, probs, 1, 0).astype(jnp.bfloat16)
        out[h] = dot(probs, order, 1, 1).astype(jnp.bfloat16)


def stash_kernel(roster, store, out):
    out[...] = store[roster[0, 15 - lax.axis_index("section")]]


def held_kernel(roster, store, came, out):
    slot = roster[1, 15 - lax.axis_index("section")]
    for i in range(store.shape[0]):
        out[i] = jnp.where(slot == i, came[...], store[i])


def part_trades(distances, values):
    return [trade(value, distance) for value, distance in zip(values, distances)]


def body(incoming, grad_in, held, roster, norm_gain, r_scores, value_weight, out_weight):
    tokens_here = incoming[0]
    grad_here = grad_in[0]
    stash_store = held[0]
    gain = norm_gain[0]
    w_value = value_weight[0]
    w_out = out_weight[0]
    width = tokens_here.shape[1]
    half = width // 2
    part = half // 2
    bf16, f32 = jnp.bfloat16, jnp.float32
    sections = lax.axis_size("section")
    ring = range(sections)
    shape = jax.ShapeDtypeStruct

    halved = [shape((ROWS // 2, half), bf16)] * 2

    def pieces(rows, came):
        return [piece for pair in zip(rows, came) for piece in pair]

    def blocks(go, stay, count):
        came = trade(go, CORE)
        return call(block_kernel, [shape((ROWS, half // count), bf16)] * count, [stay, came])

    def wide(rows):
        return [shape((rows, part), bf16)] * 2

    grads = blocks(*call(split_kernel, halved, [grad_here]), 1)[0]
    grads = call(split_join_kernel, wide(2 * ROWS), [grads, trade(grads, Z)])
    grads = call(join_kernel, wide(4 * ROWS), pieces(grads, part_trades((A, B), grads)))
    grads_came = part_trades((B, A), grads)
    normed = blocks(*call(norm_kernel, halved, [tokens_here, gain[None]]), 2)
    joined = [shape((2 * ROWS, half), bf16)]
    normed = call(join_kernel, joined, pieces(normed, part_trades((A, B), normed)))[0]
    normed = call(split_join_kernel, wide(4 * ROWS), [normed, trade(normed, Z)])
    normed_came = part_trades((B, A), normed)

    heads_width = w_out.shape[0]
    out_give = call(give_out_kernel, [shape((heads_width, half), bf16)], [w_out], mib=9)[0]
    out_other = trade(out_give, CORE)
    value_give = call(give_value_kernel, [shape((half, heads_width), bf16)], [w_value], mib=9)[0]
    value_other = trade(value_give, CORE)

    seq_len = r_scores.shape[2]
    probs = call(probs_kernel, [shape(r_scores.shape[1:], bf16)], [r_scores[0]])[0]
    probs_other = trade(probs, CORE)

    outgoing = call(stash_kernel, [shape(tokens_here.shape, bf16)], [roster.T, stash_store], smem=1)[0]
    mirrored = [(s, sections - 1 - s) for s in ring]
    arriving = lax.ppermute(tokens_here, "section", mirrored)
    fetched = lax.ppermute(outgoing, "section", mirrored)
    held_next = call(held_kernel, [shape(stash_store.shape, bf16)], [roster.T, stash_store, arriving], smem=1)[0]

    partial = [shape((seq_len, 2 * heads_width), f32)]
    rows_scratch = [pltpu.VMEM((seq_len, half), bf16)]
    mixed_scratch = [pltpu.VMEM((seq_len, 2 * heads_width), bf16)]

    def sums(rows, width):
        return [shape((rows, width), t) for t in (bf16, f32)]

    args = pieces(grads, grads_came) + [w_out, out_other]
    mine_b = call(first_b_kernel, partial, args, rows_scratch, mib=16)[0]
    args = [mine_b, trade(mine_b, CORE), probs, probs_other, w_value, value_other]
    kernel = functools.partial(second_kernel, True)
    parts_b = call(kernel, sums(4 * ROWS, part) * 2, args, mixed_scratch, mib=20)
    args = pieces(normed, normed_came) + [w_value, value_other]
    mine_f = call(first_f_kernel, partial, args, rows_scratch, mib=16)[0]
    args = [mine_f, trade(mine_f, CORE), probs, probs_other, w_out, out_other]
    kernel = functools.partial(second_kernel, False)
    parts_f = call(kernel, sums(4 * ROWS, part) * 2, args, mixed_scratch, mib=20)

    last = [shape((ROWS // 2, half), f32)] * 2
    ended = [shape(tokens_here.shape, bf16)]
    came = part_trades((A, B), parts_b[0::2])
    send, keep = call(add_kernel, sums(2 * ROWS, half), pieces(parts_b[1::2], came))
    parts = call(add_z_kernel, sums(ROWS, part) * 2, [keep, trade(send, Z)])
    came = part_trades((B, A), parts[0::2])
    go, stay = call(last_add_b_kernel, last, pieces(parts[1::2], came))
    args = [stay, trade(go, CORE), grad_here, fetched, gain[None]]
    input_grad = call(end_b_kernel, ended, args)[0]

    came = part_trades((A, B), parts_f[0::2])
    parts = call(add_kernel, sums(2 * ROWS, part) * 2, pieces(parts_f[1::2], came))
    came = part_trades((B, A), parts[0::2])
    send, keep = call(add_kernel, sums(ROWS, half), pieces(parts[1::2], came))
    go, stay = call(last_add_f_kernel, last, [keep, trade(send, Z)])
    args = [stay, trade(go, CORE), tokens_here]
    layer_out = call(end_f_kernel, ended, args)[0]
    returned = lax.ppermute(input_grad, "section", [(s, (s - 1) % sections) for s in ring])
    passed_on = lax.ppermute(layer_out, "section", [(s, (s + 1) % sections) for s in ring])
    returned = call(copy_kernel, ended, [returned])[0]
    passed_on = call(copy_kernel, ended, [passed_on])[0]
    return (passed_on[None], returned[None], held_next[None])


def solution(mesh):
    in_specs = (
        P("section", "tp", None),
        P("section", "tp", None),
        P("section", None, "tp", None),
        P(),
        P("section", None),
        P("section", "tp", None, None),
        P("section", None, "tp"),
        P("section", "tp", None),
    )
    out_specs = (P("section", "tp", None), P("section", "tp", None), P("section", None, "tp", None))

    return jax.shard_map(body, mesh=mesh, in_specs=in_specs, out_specs=out_specs, check_vma=False)
```

```python
import functools

import jax
import jax.numpy as jnp
from jax import lax
from jax.experimental import pallas as pl
from jax.experimental.pallas import tpu as pltpu
from jax.sharding import PartitionSpec as P


EPS = 0.5

A, B, Z, CORE = 4, 12, 2, 1
PLACE = {A: 1, B: 2, Z: 4}
HALVES = ((A, B), (B, A))
ROWS = 32


def trade(value, distance):
    return lax.ppermute(value, "tp", [(i, i ^ distance) for i in range(16)])


def place(order, first, second):
    return first * PLACE[order[0]] + second * PLACE[order[1]]


def row_scale(values):
    return jnp.sqrt(jnp.mean(values * values, axis=-1, keepdims=True) + EPS)


def call(kernel, outs, args, scratch=(), smem=0, mib=6):
    vmem = pl.BlockSpec(memory_space=pltpu.VMEM)
    in_specs = [pl.BlockSpec(memory_space=pltpu.SMEM)] * smem + [vmem] * (len(args) - smem)
    return pl.pallas_call(
        kernel,
        out_shape=outs,
        in_specs=in_specs,
        out_specs=[vmem] * len(outs),
        scratch_shapes=list(scratch),
        compiler_params=pltpu.CompilerParams(vmem_limit_bytes=mib * 1024 * 1024),
    )(*args)


def core_here():
    return lax.axis_index("tp") & 1


def dot(left, right, left_dim, right_dim):
    return lax.dot_general(
        left, right, (((left_dim,), (right_dim,)), ((), ())), preferred_element_type=jnp.float32
    )


def columns(start, size):
    return pl.ds(pl.multiple_of(start, 128), size)


def fill(z_first, pieces, rows):
    part = rows.shape[1] // 2
    for t, order in enumerate(HALVES):
        for late in range(2):
            for mid in range(2):
                for early in range(2):
                    first, z = (mid, early) if z_first else (early, mid)
                    to = (place(order, first, late) + z * PLACE[Z]) * ROWS
                    at = (mid * 2 + early) * ROWS
                    rows[to : to + ROWS, t * part : (t + 1) * part] = pieces[2 * t + late][at : at + ROWS, :]


def first_b_kernel(*refs):
    pieces, own, other, out, rows = refs[:4], refs[4], refs[5], refs[6], refs[7]
    fill(True, pieces, rows)
    half, heads = rows.shape[1], own.shape[0]
    out[:, :heads] = dot(rows[...], own[:, columns(core_here() * half, half)], 1, 1)
    out[:, heads:] = dot(rows[...], other[...], 1, 1)


def first_f_kernel(*refs):
    pieces, own, other, out, rows = refs[:4], refs[4], refs[5], refs[6], refs[7]
    fill(False, pieces, rows)
    half, heads = rows.shape[1], own.shape[1]
    out[:, :heads] = dot(rows[...], own[columns(core_here() * half, half), :], 1, 0)
    out[:, heads:] = dot(rows[...], other[...], 1, 0)


def mix(probs_dim, mine, theirs, probs, probs_other, mixed):
    width = mine.shape[1] // 2
    head = 128
    for half, chances in enumerate((probs, probs_other)):
        for h in range(width // head):
            at = half * width + h * head
            across = (1 - half) * width + h * head
            whole = (mine[:, at : at + head] + theirs[:, across : across + head]).astype(jnp.bfloat16)
            mixed[:, at : at + head] = dot(chances[h], whole, probs_dim, 0).astype(jnp.bfloat16)


STEP = 256


def second_kernel(bwd, mine, theirs, probs, probs_other, own, other, *refs):
    outs, mixed = refs[:4], refs[4]
    mix(0 if bwd else 1, mine, theirs, probs, probs_other, mixed)
    heads, part = other.shape[1 if bwd else 0], outs[0].shape[1]
    start = core_here() * (2 * part)
    for t, order in enumerate(HALVES):
        send, keep = outs[2 * t], outs[2 * t + 1]
        for c in range(0, part, STEP):
            at = t * part + c
            if bwd:
                total = dot(mixed[:, :heads], own[columns(start + at, STEP), :], 1, 1)
                total = total + dot(mixed[:, heads:], other[at : at + STEP, :], 1, 1)
            else:
                total = dot(mixed[:, :heads], own[:, columns(start + at, STEP)], 1, 0)
                total = total + dot(mixed[:, heads:], other[:, at : at + STEP], 1, 0)
            for mid in range(2):
                for late in range(2):
                    z, second = (mid, late) if bwd else (late, mid)
                    to = (mid * 2 + late) * ROWS
                    row = (place(order, 0, second) + z * PLACE[Z]) * ROWS
                    keep[to : to + ROWS, c : c + STEP] = total[row : row + ROWS]
                    row = (place(order, 1, second) + z * PLACE[Z]) * ROWS
                    send[to : to + ROWS, c : c + STEP] = total[row : row + ROWS].astype(jnp.bfloat16)


def add_z_kernel(kept, came, *outs):
    part = outs[0].shape[1]
    for t in range(2):
        cols = slice(t * part, (t + 1) * part)
        total = kept[:, cols] + came[:, cols].astype(jnp.float32)
        outs[2 * t][...] = total[ROWS:].astype(jnp.bfloat16)
        outs[2 * t + 1][...] = total[:ROWS]


def add_kernel(*refs):
    ins, outs = refs[:4], refs[4:]
    for t in range(2):
        kept, came = ins[2 * t], ins[2 * t + 1]
        rows = kept.shape[0] // 2
        if len(outs) == 2:
            send = outs[0].at[:, t * kept.shape[1] : (t + 1) * kept.shape[1]]
            keep = outs[1].at[:, t * kept.shape[1] : (t + 1) * kept.shape[1]]
        else:
            send, keep = outs[2 * t], outs[2 * t + 1]
        keep[...] = kept[:rows] + came[:rows].astype(jnp.float32)
        send[...] = (kept[rows:] + came[rows:].astype(jnp.float32)).astype(jnp.bfloat16)


def last_add_b_kernel(*refs):
    ins, go, stay = refs[:4], refs[4], refs[5]
    rows = ROWS // 2
    core = core_here()
    for t in range(2):
        kept, came = ins[2 * t], ins[2 * t + 1]
        part = kept.shape[1]
        for out, which in ((go, 1 - core), (stay, core)):
            at = pl.multiple_of(which * rows, rows)
            sums = kept[pl.ds(at, rows), :] + came[pl.ds(at, rows), :].astype(jnp.float32)
            out[:, t * part : (t + 1) * part] = sums


def add_f_kernel(*refs):
    ins, same, cross, go, stay = refs[:4], refs[4], refs[5], refs[6], refs[7]
    rows = ROWS // 2
    core = core_here()
    for t in range(2):
        kept, came = ins[2 * t], ins[2 * t + 1]
        part = kept.shape[1]
        for out, first, which in ((stay, 0, core), (go, 0, 1 - core), (same, ROWS, core), (cross, ROWS, 1 - core)):
            at = pl.multiple_of(first + which * rows, rows)
            sums = kept[pl.ds(at, rows), :] + came[pl.ds(at, rows), :].astype(jnp.float32)
            out[:, t * part : (t + 1) * part] = sums.astype(out.dtype)


def split_kernel(rows, go, stay):
    half = go.shape[1]
    lower = core_here() == 0
    go[...] = jnp.where(lower, rows[:, half:], rows[:, :half])
    stay[...] = jnp.where(lower, rows[:, :half], rows[:, half:])


def norm_kernel(rows, gain, go, stay):
    half = go.shape[1]
    values = rows[...].astype(jnp.float32)
    normed = (values / row_scale(values) * gain[...]).astype(jnp.bfloat16)
    lower = core_here() == 0
    go[...] = jnp.where(lower, normed[:, half:], normed[:, :half])
    stay[...] = jnp.where(lower, normed[:, :half], normed[:, half:])


def block_kernel(stay, came, *outs):
    rows, part = stay.shape[0], outs[0].shape[1]
    lower = core_here() == 0
    for t, out in enumerate(outs):
        mine, other = stay[:, t * part : (t + 1) * part], came[:, t * part : (t + 1) * part]
        out[:rows] = jnp.where(lower, mine, other)
        out[rows:] = jnp.where(lower, other, mine)


def split_join_kernel(had, came, *outs):
    rows, part = had.shape[0], outs[0].shape[1]
    for t, out in enumerate(outs):
        out[:rows] = had[:, t * part : (t + 1) * part]
        out[rows:] = came[:, t * part : (t + 1) * part]


def join_kernel(*refs):
    ins, outs = refs[:4], refs[4:]
    for t in range(2):
        had, came = ins[2 * t], ins[2 * t + 1]
        rows, part = had.shape
        out = outs[t] if len(outs) == 2 else outs[0].at[:, t * part : (t + 1) * part]
        out[:rows] = had[...]
        out[rows:] = came[...]


def copy_kernel(value, out):
    out[...] = value[...]


def whole(stay, came):
    lower = core_here() == 0
    return jnp.concatenate(
        [jnp.where(lower, stay[...], came[...]), jnp.where(lower, came[...], stay[...])], axis=1
    )


def end_f_kernel(stay, same, kept, cross, tokens, out):
    own = stay[...] + same[...].astype(jnp.float32)
    other = kept[...] + cross[...].astype(jnp.float32)
    lower = core_here() == 0
    sums = jnp.concatenate([jnp.where(lower, own, other), jnp.where(lower, other, own)], axis=1)
    out[...] = (tokens[...].astype(jnp.float32) + sums).astype(jnp.bfloat16)


def end_b_kernel(stay, came, grads, stash, gain, out):
    weighted = gain[...] * whole(stay, came)
    stash_f32 = stash[...].astype(jnp.float32)
    scale = row_scale(stash_f32)
    inner_sum = jnp.sum(weighted * stash_f32, axis=-1, keepdims=True)
    width = stash_f32.shape[1]
    out[...] = (
        grads[...].astype(jnp.float32) + weighted / scale - stash_f32 * inner_sum / (width * (scale * scale * scale))
    ).astype(jnp.bfloat16)


def give_out_kernel(weights, out):
    half = out.shape[1]
    out[...] = weights[:, columns((1 - core_here()) * half, half)]


def give_value_kernel(weights, out):
    half = out.shape[0]
    out[...] = weights[columns((1 - core_here()) * half, half), :]


def probs_kernel(scores, out):
    length = scores.shape[1]
    row = lax.broadcasted_iota(jnp.int32, (length, length), 0)
    col = lax.broadcasted_iota(jnp.int32, (length, length), 1)
    tp = lax.axis_index("tp")
    at = row >> 5
    token = (((tp >> 2) ^ (at & 1) ^ (((at >> 1) & 1) * 3)) << 6) | ((((tp >> 1) & 1) ^ (at >> 2)) << 5) | (row & 31)
    order = (token == col).astype(jnp.bfloat16)
    allowed = col <= row
    for h in range(scores.shape[0]):
        masked = jnp.where(allowed, scores[h], -jnp.inf)
        highest = jnp.max(masked, axis=-1, keepdims=True)
        expo = jnp.exp(masked - highest)
        probs = (expo / jnp.sum(expo, axis=-1, keepdims=True)).astype(jnp.bfloat16)
        probs = dot(order, probs, 1, 0).astype(jnp.bfloat16)
        out[h] = dot(probs, order, 1, 1).astype(jnp.bfloat16)


def stash_kernel(roster, store, out):
    out[...] = store[roster[0, 15 - lax.axis_index("section")]]


def held_kernel(roster, store, came, out):
    slot = roster[1, 15 - lax.axis_index("section")]
    for i in range(store.shape[0]):
        out[i] = jnp.where(slot == i, came[...], store[i])


def part_trades(distances, values):
    return [trade(value, distance) for value, distance in zip(values, distances)]


def body(incoming, grad_in, held, roster, norm_gain, r_scores, value_weight, out_weight):
    tokens_here = incoming[0]
    grad_here = grad_in[0]
    stash_store = held[0]
    gain = norm_gain[0]
    w_value = value_weight[0]
    w_out = out_weight[0]
    width = tokens_here.shape[1]
    half = width // 2
    part = half // 2
    bf16, f32 = jnp.bfloat16, jnp.float32
    sections = lax.axis_size("section")
    ring = range(sections)
    shape = jax.ShapeDtypeStruct

    halved = [shape((ROWS // 2, half), bf16)] * 2

    def pieces(rows, came):
        return [piece for pair in zip(rows, came) for piece in pair]

    def blocks(go, stay, count):
        came = trade(go, CORE)
        return call(block_kernel, [shape((ROWS, half // count), bf16)] * count, [stay, came])

    def wide(rows):
        return [shape((rows, part), bf16)] * 2

    grads = blocks(*call(split_kernel, halved, [grad_here]), 1)[0]
    grads = call(split_join_kernel, wide(2 * ROWS), [grads, trade(grads, Z)])
    grads = call(join_kernel, wide(4 * ROWS), pieces(grads, part_trades((A, B), grads)))
    grads_came = part_trades((B, A), grads)
    normed = blocks(*call(norm_kernel, halved, [tokens_here, gain[None]]), 2)
    joined = [shape((2 * ROWS, half), bf16)]
    normed = call(join_kernel, joined, pieces(normed, part_trades((A, B), normed)))[0]
    normed = call(split_join_kernel, wide(4 * ROWS), [normed, trade(normed, Z)])
    normed_came = part_trades((B, A), normed)

    heads_width = w_out.shape[0]
    out_give = call(give_out_kernel, [shape((heads_width, half), bf16)], [w_out], mib=9)[0]
    out_other = trade(out_give, CORE)
    value_give = call(give_value_kernel, [shape((half, heads_width), bf16)], [w_value], mib=9)[0]
    value_other = trade(value_give, CORE)

    seq_len = r_scores.shape[2]
    probs = call(probs_kernel, [shape(r_scores.shape[1:], bf16)], [r_scores[0]])[0]
    probs_other = trade(probs, CORE)

    outgoing = call(stash_kernel, [shape(tokens_here.shape, bf16)], [roster.T, stash_store], smem=1)[0]
    mirrored = [(s, sections - 1 - s) for s in ring]
    arriving = lax.ppermute(tokens_here, "section", mirrored)
    fetched = lax.ppermute(outgoing, "section", mirrored)
    held_next = call(held_kernel, [shape(stash_store.shape, bf16)], [roster.T, stash_store, arriving], smem=1)[0]

    partial = [shape((seq_len, 2 * heads_width), f32)]
    rows_scratch = [pltpu.VMEM((seq_len, half), bf16)]
    mixed_scratch = [pltpu.VMEM((seq_len, 2 * heads_width), bf16)]

    def sums(rows, width):
        return [shape((rows, width), t) for t in (bf16, f32)]

    args = pieces(grads, grads_came) + [w_out, out_other]
    mine_b = call(first_b_kernel, partial, args, rows_scratch, mib=16)[0]
    args = [mine_b, trade(mine_b, CORE), probs, probs_other, w_value, value_other]
    kernel = functools.partial(second_kernel, True)
    parts_b = call(kernel, sums(4 * ROWS, part) * 2, args, mixed_scratch, mib=20)
    args = pieces(normed, normed_came) + [w_value, value_other]
    mine_f = call(first_f_kernel, partial, args, rows_scratch, mib=16)[0]
    args = [mine_f, trade(mine_f, CORE), probs, probs_other, w_out, out_other]
    kernel = functools.partial(second_kernel, False)
    parts_f = call(kernel, sums(4 * ROWS, part) * 2, args, mixed_scratch, mib=20)

    last = [shape((ROWS // 2, half), f32)] * 2
    ended = [shape(tokens_here.shape, bf16)]
    came = part_trades((A, B), parts_b[0::2])
    send, keep = call(add_kernel, sums(2 * ROWS, half), pieces(parts_b[1::2], came))
    parts = call(add_z_kernel, sums(ROWS, part) * 2, [keep, trade(send, Z)])
    came = part_trades((B, A), parts[0::2])
    go, stay = call(last_add_b_kernel, last, pieces(parts[1::2], came))
    args = [stay, trade(go, CORE), grad_here, fetched, gain[None]]
    input_grad = call(end_b_kernel, ended, args)[0]

    came = part_trades((A, B), parts_f[0::2])
    parts = call(add_kernel, sums(2 * ROWS, part) * 2, pieces(parts_f[1::2], came))
    came = part_trades((B, A), parts[0::2])
    ends = [shape((ROWS // 2, half), t) for t in (bf16, bf16, f32, f32)]
    same, cross, go, stay = call(add_f_kernel, ends, pieces(parts[1::2], came))
    args = [stay, trade(same, Z), trade(go, CORE), trade(cross, Z | CORE), tokens_here]
    layer_out = call(end_f_kernel, ended, args)[0]
    returned = lax.ppermute(input_grad, "section", [(s, (s - 1) % sections) for s in ring])
    passed_on = lax.ppermute(layer_out, "section", [(s, (s + 1) % sections) for s in ring])
    returned = call(copy_kernel, ended, [returned])[0]
    passed_on = call(copy_kernel, ended, [passed_on])[0]
    return (passed_on[None], returned[None], held_next[None])


def solution(mesh):
    in_specs = (
        P("section", "tp", None),
        P("section", "tp", None),
        P("section", None, "tp", None),
        P(),
        P("section", None),
        P("section", "tp", None, None),
        P("section", None, "tp"),
        P("section", "tp", None),
    )
    out_specs = (P("section", "tp", None), P("section", "tp", None), P("section", None, "tp", None))

    return jax.shard_map(body, mesh=mesh, in_specs=in_specs, out_specs=out_specs, check_vma=False)
```
